32 devices in a mesh: grp: 4 (over y, core), dev: 8 (over z, x).
Axes of the slice: x: 2, y: 2, z: 4, core: 2. Of those that a mesh axis runs over, the one named last changes fastest.
Arguments:
- old_fine: float32 [512, 9, 64, 128], P('dev', None, 'grp'), may hold values from -6 to 6
- old_ids: int32 [4, 512], P('grp', 'dev'), may hold values from -1 to 511, as said below
- old_coarse: float32 [256, 9, 32, 64], P('dev', None, 'grp'), may hold values from -6 to 6
- coarse_ids: int32 [4, 256], P('grp', 'dev'), may hold values from 0 to 255, as said below
- velocity: float32 [512, 3, 64, 128], P('dev', None, 'grp'), may hold values from -0.12 to 0.12
- diffusion: float32 [9], replicated, may hold values from 0.01 to 0.1
Outputs:
- species_out: float32 [512, 9, 64, 128], P('dev', None, 'grp')
The draws below stay inside these ranges and needn't reach their ends.
Inputs may be any that keep to these rules, and one draw needn't show every extreme that they name: `old_ids`: row g names, for each old fine slot k of group g (on dev index k // 64), the x-plane that the slot holds, or -1 for an empty slot whose rows of old_fine are ignored. No plane is named twice; planes named nowhere are newly refined. The slots of one device hold at most 16 planes of any one new box, box e holding planes e * 64 to e * 64 + 63. `coarse_ids`: each row is a permutation. The slots of one device hold at most 8 of the coarse planes e * 32 to e * 32 + 31 of any one new box e.
All inputs are finite; a program needn't handle non-finite values.
Results may differ from the reference program's by a relative error of at most 0.000092.
Values sent between devices are 32-bit elements; how exact they have to be, the bound alone decides.
A program may use at most 192 MiB of HBM per device.

```python
import math
import jax
import jax.numpy as jnp

S = 9
BX = 64
BY = 16
BZ = 128
ITERS = 2
CAP = 16
CBX = 32
CCAP = 8
NX = 512
NY = 64
CX = 256
CY = 32
CZ = 64
N_GRP = 4
N_DEV = 8


def regrid_map(key, block_len, capacity, with_empty):
    rows_out = []
    for group_index in range(N_GRP):
        group_key = jax.random.fold_in(key, group_index)
        key_order = jax.random.fold_in(group_key, 1)
        key_offset = jax.random.fold_in(group_key, 2)
        key_slots = jax.random.fold_in(group_key, 3)
        key_level = jax.random.fold_in(group_key, 4)
        key_rolls = jax.random.fold_in(group_key, 5)
        placing = jax.random.permutation(key_order, N_DEV)
        shuffled = jax.random.permutation(key_offset, capacity * N_DEV) // capacity
        first_value = shuffled[0]
        scores = jnp.where(shuffled == first_value, 1, 0).astype(jnp.int32)
        reorder = jnp.argsort(scores, stable=True)
        rest_values = shuffled[reorder][:block_len - capacity]
        offsets = jnp.concatenate([jnp.full((capacity,), first_value, jnp.int32), rest_values.astype(jnp.int32)])
        slot_order = jax.random.permutation(key_slots, block_len)
        boxes = jnp.arange(N_DEV, dtype=jnp.int32)[:, None]
        planes = jnp.arange(block_len, dtype=jnp.int32)[None, :]
        holder = (placing[:, None] + offsets[None, :]) % N_DEV
        positions = holder * block_len + slot_order[None, :]
        values = boxes * block_len + planes
        if with_empty:
            levels = jax.random.randint(key_level, (N_DEV,), 0, 5)
            rolls = jax.random.randint(key_rolls, (N_DEV, block_len), 0, 8)
            fresh_mask = (rolls < levels[:, None]) & jnp.logical_not((boxes == 0) & (planes < capacity))
            values = jnp.where(fresh_mask, -1, values)
        row_values = jnp.zeros((N_DEV * block_len,), jnp.int32).at[positions.reshape(-1)].set(values.reshape(-1).astype(jnp.int32))
        rows_out.append(row_values)
    return jnp.stack(rows_out, axis=0)


def draw_old_ids(key, part):
    return regrid_map(jax.random.fold_in(key, 11), BX, CAP, True)


def draw_coarse_ids(key, part):
    return regrid_map(jax.random.fold_in(key, 23), CBX, CCAP, False)


def level_of(stream_key, shape, split, smallest, high):
    loudness, own = 1.0, jax.random.fold_in(stream_key, 6)
    for axis_at, parts in split:
        heights = jnp.exp(jax.random.uniform(jax.random.fold_in(own, axis_at), (parts,), jnp.float32, smallest / len(split), high / len(split)))
        loudness = loudness * jnp.repeat(heights, shape[axis_at] // parts).reshape([-1 if axis == axis_at else 1 for axis in range(len(shape))])
    return loudness


def gaussian(own_key, dims, spread, reach, cuts=(), kind=jnp.bfloat16):
    loudness = level_of(own_key, dims, cuts, -0.22, 0.18) if cuts else 1.0
    array = jax.random.normal(own_key, dims, jnp.float32) * spread * loudness
    return jnp.minimum(jnp.maximum(array, -reach), reach).astype(kind)


def setup_inputs(seed: int = 0) -> dict:
    arg_keys = jax.random.split(jax.random.key(seed), 7)
    old_fine = gaussian(arg_keys[0], (NX, S, NY, BZ), 1.0, 6.0, ((0, 8), (2, 4)), jnp.float32)
    old_ids = draw_old_ids(jax.random.fold_in(arg_keys[6], 71), 0)
    old_coarse = gaussian(arg_keys[2], (CX, S, CY, CZ), 1.0, 6.0, ((0, 8), (2, 4)), jnp.float32)
    coarse_ids = draw_coarse_ids(jax.random.fold_in(arg_keys[6], 71), 0)
    velocity = gaussian(arg_keys[4], (NX, 3, NY, BZ), 0.045, 0.12, ((0, 8), (2, 4)), jnp.float32)
    diffusion = jnp.clip(jnp.exp(jax.random.uniform(arg_keys[5], (S,), jnp.float32, math.log(0.01), math.log(0.1))), 0.01, 0.1)
    return dict(old_fine=old_fine, old_ids=old_ids, old_coarse=old_coarse, coarse_ids=coarse_ids, velocity=velocity, diffusion=diffusion)


def refine(coarse):
    extent = coarse.shape
    ypadded = jnp.concatenate([coarse[:, :, :1], coarse, coarse[:, :, -1:]], axis=2)
    zpadded = jnp.concatenate([coarse[..., :1], coarse, coarse[..., -1:]], axis=3)
    slope_y = 0.5 * (ypadded[:, :, 2:] - ypadded[:, :, :-2])
    slope_z = 0.5 * (zpadded[..., 2:] - zpadded[..., :-2])
    row_parts = []
    for row_half in range(2):
        col_parts = [coarse + (0.5 * row_half - 0.25) * slope_y + (0.5 * col_half - 0.25) * slope_z for col_half in range(2)]
        row_parts.append(jnp.stack(col_parts, axis=-1))
    children = jnp.stack(row_parts, axis=3)
    refined = children.reshape(extent[0], extent[1], 2 * extent[2], 2 * extent[3])
    return jnp.repeat(refined, 2, axis=0)


def advance(padded, flow_field, diffusion):
    center = padded[1:-1, :, 1:-1]
    zpadded = jnp.concatenate([center[..., :1], center, center[..., -1:]], axis=3)
    minus_side = [padded[:-2, :, 1:-1], padded[1:-1, :, :-2], zpadded[..., :-2]]
    plus_side = [padded[2:, :, 1:-1], padded[1:-1, :, 2:], zpadded[..., 2:]]
    laplace = minus_side[0] + plus_side[0] + minus_side[1] + plus_side[1] + minus_side[2] + plus_side[2] - 6.0 * center
    transport = jnp.zeros_like(center)
    for direction in range(3):
        speed_part = flow_field[:, direction:direction + 1]
        transport = transport + jnp.maximum(speed_part, 0.0) * (center - minus_side[direction]) + jnp.minimum(speed_part, 0.0) * (plus_side[direction] - center)
    return center + diffusion[None, :, None, None] * laplace - transport


def reference(old_fine, old_ids, old_coarse, coarse_ids, velocity, diffusion):
    pieces = []
    half_rows = BY // 2
    for group_index in range(N_GRP):
        labels = old_ids[group_index]
        target = jnp.where(labels >= 0, labels, NX).astype(jnp.int32)
        source = jnp.full((NX,), -1, jnp.int32).at[target].set(jnp.arange(NX, dtype=jnp.int32), mode="drop")
        moved_rows = old_fine[jnp.maximum(source, 0).astype(jnp.int32), :, group_index * BY:(group_index + 1) * BY]
        coarse_source = jnp.zeros((CX,), jnp.int32).at[coarse_ids[group_index].astype(jnp.int32)].set(jnp.arange(CX, dtype=jnp.int32))
        parents = old_coarse[coarse_source, :, group_index * half_rows:(group_index + 1) * half_rows]
        interp = refine(parents)
        pieces.append(jnp.where((source < 0)[:, None, None, None], interp, moved_rows))
    species_state = jnp.concatenate(pieces, axis=2)
    for repeat in range(ITERS):
        padded = jnp.pad(species_state, ((1, 1), (0, 0), (1, 1), (0, 0)))
        species_state = advance(padded, velocity, diffusion)
    return species_state
```

```python
import functools

import jax
import jax.numpy as jnp
from jax import lax
from jax.experimental import pallas as pl
from jax.experimental.pallas import tpu as pltpu
from jax.sharding import PartitionSpec as P

ITERS = 2
VMEM_LIMIT = 48 * 1024 * 1024


def params(**more):
    return pltpu.CompilerParams(vmem_limit_bytes=VMEM_LIMIT, **more)


def earlier_count(mask):
    count = mask.shape[-1]
    lower = jnp.arange(count)[None, :] < jnp.arange(count)[:, None]
    return jnp.sum((mask[..., None, :] & lower).astype(jnp.int32), axis=-1)


def send_table(labels, block_len, devices, capacity):
    target = jnp.where(labels >= 0, labels // block_len, -1)
    count = labels.shape[0]
    same = target[None, :] == target[:, None]
    lower = jnp.arange(count)[None, :] < jnp.arange(count)[:, None]
    rank = jnp.sum((same & lower).astype(jnp.int32), axis=1)
    slot = jnp.where(labels >= 0, target * capacity + rank, -1)
    hits = slot[None, :] == jnp.arange(devices * capacity)[:, None]
    return jnp.max(jnp.where(hits, jnp.arange(count)[None, :], 0), axis=1)


def receive_table(labels_all, block_len, capacity, me):
    devices, count = labels_all.shape
    within = labels_all - me * block_len
    valid = (within >= 0) & (within < block_len)
    slot = jnp.arange(devices)[:, None] * capacity + earlier_count(valid)
    flat_within = jnp.where(valid, within, -1).reshape(-1)
    hits = flat_within[None, :] == jnp.arange(block_len)[:, None]
    return jnp.max(jnp.where(hits, slot.reshape(-1)[None, :], -1), axis=1)


def pack_fine_kernel(table, source, out, sem):
    def send(i, carry):
        pltpu.make_async_copy(source.at[table[i]], out.at[i], sem).start()
        return carry

    lax.fori_loop(0, out.shape[0], send, 0)
    pltpu.make_async_copy(out, out, sem).wait()


def pack_fine(table, fine):
    return pl.pallas_call(
        pack_fine_kernel,
        out_shape=jax.ShapeDtypeStruct((table.shape[0],) + fine.shape[1:], fine.dtype),
        in_specs=[
            pl.BlockSpec(memory_space=pltpu.SMEM),
            pl.BlockSpec(memory_space=pltpu.VMEM),
        ],
        out_specs=pl.BlockSpec(memory_space=pl.ANY),
        scratch_shapes=[pltpu.SemaphoreType.DMA],
        compiler_params=params(),
        name="pack_fine",
    )(table, fine)


def pack_coarse_kernel(table, source, out):
    half = source.shape[-1]

    def step(i, carry):
        out[i, :, :, 0:half] = source[table[2 * i]]
        out[i, :, :, half : 2 * half] = source[table[2 * i + 1]]
        return carry

    lax.fori_loop(0, out.shape[0], step, 0)


def pack_coarse(table, coarse):
    shape = (table.shape[0] // 2,) + coarse.shape[1:3] + (2 * coarse.shape[3],)
    return pl.pallas_call(
        pack_coarse_kernel,
        out_shape=jax.ShapeDtypeStruct(shape, coarse.dtype),
        in_specs=[
            pl.BlockSpec(memory_space=pltpu.SMEM),
            pl.BlockSpec(memory_space=pltpu.VMEM),
        ],
        out_specs=pl.BlockSpec(memory_space=pltpu.VMEM),
        compiler_params=params(),
        name="pack_coarse",
    )(table, coarse)


def refine_kernel(table, pairs, weights, out):
    species, rows, depth = pairs.shape[1:]
    half = depth // 2
    lane = lax.broadcasted_iota(jnp.int32, (species * rows, depth), 1)
    row = lax.broadcasted_iota(jnp.int32, (species, rows, depth), 1)

    def step(c, carry):
        slot = jnp.maximum(table[c], 0)
        block = pairs[slot // 2].reshape(species * rows, depth)
        odd = slot % 2
        block = jnp.where((lane >= half).astype(jnp.int32) == odd, block, 0.0)
        spread = jnp.dot(
            block, weights[...], precision=lax.Precision.HIGHEST,
            preferred_element_type=jnp.float32,
        )
        plain = spread[:, :depth].reshape(species, rows, depth)
        sloped = spread[:, depth:].reshape(species, rows, depth)
        below = jnp.where(row == 0, plain, pltpu.roll(plain, 1, 1))
        above = jnp.where(row == rows - 1, plain, pltpu.roll(plain, rows - 1, 1))
        slope = 0.125 * (above - below)
        for s in range(species):
            out[c, s, pl.ds(0, rows, 2), :] = sloped[s] - slope[s]
            out[c, s, pl.ds(1, rows, 2), :] = sloped[s] + slope[s]
        return carry

    lax.fori_loop(0, out.shape[0], step, 0)


def spread_weights(half):
    depth = 2 * half
    coarse = jnp.arange(half)[:, None]
    fine = jnp.arange(depth)[None, :]
    centre = (fine // 2 == coarse).astype(jnp.float32)
    up = (jnp.minimum(fine // 2 + 1, half - 1) == coarse).astype(jnp.float32)
    down = (jnp.maximum(fine // 2 - 1, 0) == coarse).astype(jnp.float32)
    side = jnp.where(fine % 2 == 1, 0.125, -0.125)
    both = jnp.concatenate([centre, centre + side * (up - down)], axis=1)
    return jnp.concatenate([both, both], axis=0)


def refine(table, pairs, weights):
    species, rows, depth = pairs.shape[1:]
    return pl.pallas_call(
        refine_kernel,
        out_shape=jax.ShapeDtypeStruct(
            (table.shape[0], species, 2 * rows, depth), pairs.dtype
        ),
        in_specs=[
            pl.BlockSpec(memory_space=pltpu.SMEM),
            pl.BlockSpec(memory_space=pltpu.VMEM),
            pl.BlockSpec(memory_space=pltpu.VMEM),
        ],
        out_specs=pl.BlockSpec(memory_space=pltpu.VMEM),
        compiler_params=params(),
        cost_estimate=pl.CostEstimate(
            flops=40_000_000, bytes_accessed=30_000_000, transcendentals=0
        ),
        name="refine",
    )(table, pairs, weights)


def assemble_kernel(table, arrived, interp, out, low, high, sem):
    planes = out.shape[0]
    rows = out.shape[2]

    def fetch(p, carry):
        slot = table[p]

        @pl.when(slot >= 0)
        def _():
            pltpu.make_async_copy(arrived.at[slot], out.at[p], sem).start()

        @pl.when(slot < 0)
        def _():
            pltpu.make_async_copy(interp.at[p // 2], out.at[p], sem).start()

        return carry

    lax.fori_loop(0, planes, fetch, 0)
    pltpu.make_async_copy(out, out, sem).wait()

    def edges(p, carry):
        low[p] = out[p, :, 0, :]
        high[p] = out[p, :, rows - 1, :]
        return carry

    lax.fori_loop(0, planes, edges, 0)


def assemble(table, arrived, interp):
    planes = table.shape[0]
    species, rows, depth = arrived.shape[1:]
    edge = jax.ShapeDtypeStruct((planes, species, depth), arrived.dtype)
    return pl.pallas_call(
        assemble_kernel,
        out_shape=(
            jax.ShapeDtypeStruct((planes, species, rows, depth), arrived.dtype),
            edge,
            edge,
        ),
        in_specs=[
            pl.BlockSpec(memory_space=pltpu.SMEM),
            pl.BlockSpec(memory_space=pl.ANY),
            pl.BlockSpec(memory_space=pl.ANY),
        ],
        out_specs=(pl.BlockSpec(memory_space=pltpu.VMEM),) * 3,
        scratch_shapes=[pltpu.SemaphoreType.DMA],
        compiler_params=params(),
        name="assemble",
    )(table, arrived, interp)


def advance_kernel(steps, diffusion, u, before, after, first, last, below, above, flow, out, *edges):
    i = pl.program_id(0)
    block, species, rows, depth = u.shape
    row = lax.broadcasted_iota(jnp.int32, (rows, depth), 0)
    lane = lax.broadcasted_iota(jnp.int32, (rows, depth), 1)

    def plane(x, s):
        return u[x, s]

    for x in range(block):
        v = [flow[x, k] for k in range(3)]
        plus = [jnp.maximum(w, 0.0) for w in v]
        minus = [jnp.maximum(-w, 0.0) for w in v]
        rest = 1.0
        for k in range(3):
            rest = rest - plus[k] - minus[k]
        for s in range(species):
            d = diffusion[s]
            c = u[x, s]
            if x > 0:
                lo = u[x - 1, s]
            else:
                lo = jnp.where(i == 0, first[0, s], before[0, s])
            if x < block - 1:
                hi = u[x + 1, s]
            else:
                hi = jnp.where(i == steps - 1, last[0, s], after[0, s])
            ylo = jnp.where(row == 0, below[x, pl.ds(s, 1), :], pltpu.roll(c, 1, 0))
            yhi = jnp.where(row == rows - 1, above[x, pl.ds(s, 1), :], pltpu.roll(c, rows - 1, 0))
            zlo = jnp.where(lane == 0, c, pltpu.roll(c, 1, 1))
            zhi = jnp.where(lane == depth - 1, c, pltpu.roll(c, depth - 1, 1))
            total = (rest - 6.0 * d) * c
            total = total + (plus[0] + d) * lo + (minus[0] + d) * hi
            total = total + (plus[1] + d) * ylo + (minus[1] + d) * yhi
            total = total + (plus[2] + d) * zlo + (minus[2] + d) * zhi
            out[x, s] = total
            if edges:
                edges[0][x, pl.ds(s, 1), :] = total[0:1]
                edges[1][x, pl.ds(s, 1), :] = total[rows - 1 : rows]


def advance(diffusion, u, first, last, below, above, flow, with_edges):
    planes, species, rows, depth = u.shape
    block = 8 if planes % 8 == 0 else 1
    steps = planes // block
    edge_spec = pl.BlockSpec((block, species, depth), lambda i: (i, 0, 0))
    plane_spec = pl.BlockSpec((1, species, rows, depth), lambda i: (0, 0, 0, 0))
    block_spec = pl.BlockSpec((block, species, rows, depth), lambda i: (i, 0, 0, 0))
    shapes = [jax.ShapeDtypeStruct(u.shape, u.dtype)]
    out_specs = [block_spec]
    if with_edges:
        shapes += [jax.ShapeDtypeStruct((planes, species, depth), u.dtype)] * 2
        out_specs += [edge_spec] * 2
    return pl.pallas_call(
        functools.partial(advance_kernel, steps),
        grid=(steps,),
        out_shape=shapes,
        in_specs=[
            pl.BlockSpec(memory_space=pltpu.SMEM),
            block_spec,
            pl.BlockSpec(
                (1, species, rows, depth), lambda i: (jnp.maximum(i * block - 1, 0), 0, 0, 0)
            ),
            pl.BlockSpec(
                (1, species, rows, depth),
                lambda i: (jnp.minimum(i * block + block, planes - 1), 0, 0, 0),
            ),
            plane_spec,
            plane_spec,
            edge_spec,
            edge_spec,
            pl.BlockSpec((block, 3, rows, depth), lambda i: (i, 0, 0, 0)),
        ],
        out_specs=out_specs,
        compiler_params=params(),
        name="advance",
    )(diffusion, u, u, u, first, last, below, above, flow)


def shift_up(value, axis):
    size = lax.axis_size(axis)
    return lax.ppermute(value, axis, [(i, i + 1) for i in range(size - 1)])


def shift_down(value, axis):
    size = lax.axis_size(axis)
    return lax.ppermute(value, axis, [(i + 1, i) for i in range(size - 1)])


def on_device(old_fine, old_ids, old_coarse, coarse_ids, velocity, diffusion):
    devices = lax.axis_size("dev")
    me = lax.axis_index("dev")
    planes = old_fine.shape[0]
    coarse_planes = old_coarse.shape[0]
    capacity = max(2, 2 * planes // devices)
    coarse_capacity = max(2, 2 * coarse_planes // devices)
    both = jnp.concatenate([old_ids[0], coarse_ids[0]])
    both_all = lax.all_gather(both, "dev")
    fine_send = send_table(old_ids[0], planes, devices, capacity)
    coarse_send = send_table(coarse_ids[0], coarse_planes, devices, coarse_capacity)
    coarse_out = pack_coarse(coarse_send, old_coarse)
    coarse_in = lax.all_to_all(coarse_out, "dev", split_axis=0, concat_axis=0, tiled=True)
    fine_out = pack_fine(fine_send, old_fine)
    fine_in = lax.all_to_all(fine_out, "dev", split_axis=0, concat_axis=0, tiled=True)
    fine_table = receive_table(both_all[:, :planes], planes, capacity, me)
    coarse_table = receive_table(both_all[:, planes:], coarse_planes, coarse_capacity, me)
    interp = refine(coarse_table, coarse_in, spread_weights(old_coarse.shape[3]))
    u, low, high = assemble(fine_table, fine_in, interp)
    for repeat in range(ITERS):
        first = shift_up(u[-1:], "dev")
        last = shift_down(u[:1], "dev")
        below = shift_up(high, "grp")
        above = shift_down(low, "grp")
        more = repeat < ITERS - 1
        outs = advance(diffusion, u, first, last, below, above, velocity, more)
        if more:
            u, low, high = outs
        else:
            u = outs[0]
    return u


def solution(mesh):
    in_specs = (
        P("dev", None, "grp", None),
        P("grp", "dev"),
        P("dev", None, "grp", None),
        P("grp", "dev"),
        P("dev", None, "grp", None),
        P(),
    )
    out_specs = P("dev", None, "grp", None)
    return jax.shard_map(
        on_device, mesh=mesh, in_specs=in_specs, out_specs=out_specs, check_vma=False
    )
```

```python
import functools

import jax
import jax.numpy as jnp
from jax import lax
from jax.experimental import pallas as pl
from jax.experimental.pallas import tpu as pltpu
from jax.sharding import PartitionSpec as P

ITERS = 2
VMEM_LIMIT = 48 * 1024 * 1024


def params(**more):
    return pltpu.CompilerParams(vmem_limit_bytes=VMEM_LIMIT, **more)


def earlier_count(mask):
    count = mask.shape[-1]
    lower = jnp.arange(count)[None, :] < jnp.arange(count)[:, None]
    return jnp.sum((mask[..., None, :] & lower).astype(jnp.int32), axis=-1)


def send_table(labels, block_len, devices, capacity):
    target = jnp.where(labels >= 0, labels // block_len, -1)
    count = labels.shape[0]
    same = target[None, :] == target[:, None]
    lower = jnp.arange(count)[None, :] < jnp.arange(count)[:, None]
    rank = jnp.sum((same & lower).astype(jnp.int32), axis=1)
    slot = jnp.where(labels >= 0, target * capacity + rank, -1)
    hits = slot[None, :] == jnp.arange(devices * capacity)[:, None]
    return jnp.max(jnp.where(hits, jnp.arange(count)[None, :], 0), axis=1)


def receive_table(labels_all, block_len, capacity, me):
    devices, count = labels_all.shape
    within = labels_all - me * block_len
    valid = (within >= 0) & (within < block_len)
    slot = jnp.arange(devices)[:, None] * capacity + earlier_count(valid)
    flat_within = jnp.where(valid, within, -1).reshape(-1)
    hits = flat_within[None, :] == jnp.arange(block_len)[:, None]
    return jnp.max(jnp.where(hits, slot.reshape(-1)[None, :], -1), axis=1)


def pair_count(same):
    count = same.shape[-1]
    lower = jnp.arange(count)[None, :] < jnp.arange(count)[:, None]
    return jnp.sum((same & lower).astype(jnp.int32), axis=-1)


def exchange_plan(labels, block_len, first_cap, second_cap):
    devices = labels.shape[0]
    part = devices // 2
    owners = jnp.arange(devices)
    valid = labels >= 0
    owner = jnp.where(valid, labels // block_len, -1)
    rank = pair_count(owner[:, None, :] == owner[:, :, None])
    over = valid & (rank >= first_cap)
    half = owner // part
    order = pair_count(over[:, None, :] & (half[:, None, :] == half[:, :, None]))
    counts = jnp.sum((owner[:, :, None] == owners).astype(jnp.int32), axis=1)
    spot = jnp.arange(first_cap)
    free = (spot >= counts[:, :, None]).astype(jnp.int32)
    by_half = free.reshape(devices, 2, part, first_cap)
    level = jnp.sum(by_half, axis=2)
    higher = jnp.sum(jnp.where(spot[None, :] > spot[:, None], level[:, :, None, :], 0), axis=-1)
    member = jnp.arange(part)
    beside = jnp.sum(
        jnp.where((member[None, :] < member[:, None])[:, :, None], by_half[:, :, None], 0), axis=3
    )
    at = jnp.where(by_half > 0, higher[:, :, None, :] + beside, -1)
    at = at.reshape(devices, 1, devices * first_cap)
    spots = jnp.arange(devices * first_cap)
    match = (at == order[:, :, None]) & ((spots // first_cap) // part == half[:, :, None])
    borrowed = jnp.max(jnp.where(match, spots, -1), axis=-1)
    slot = jnp.where(valid, jnp.where(over, borrowed, owner * first_cap + rank), -1)
    via = slot // first_cap
    relayed = over & (via != owner)
    lane = jnp.where(relayed, via * part + owner % part, -1)
    within = pair_count(lane[:, None, :] == lane[:, :, None])
    lanes = jnp.arange(devices * part)
    per_source = jnp.sum((lane[:, :, None] == lanes).astype(jnp.int32), axis=1)
    ahead = jnp.sum(
        jnp.where((owners[None, :] < owners[:, None])[:, :, None], per_source[None], 0), axis=1
    )
    mine = lane[:, :, None] == lanes
    second = within + jnp.sum(jnp.where(mine, ahead[:, None, :], 0), axis=-1)
    fits = jnp.all(jnp.where(over, borrowed >= 0, True))
    fits = fits & jnp.all(jnp.sum(per_source, axis=0) <= second_cap)
    return owner, slot, relayed, second, fits


def plan_tables(labels, plan, block_len, first_cap, second_cap, me):
    owner, slot, relayed, second, _ = plan
    devices, count = labels.shape
    part = devices // 2
    via = slot // first_cap
    mine = jnp.max(jnp.where(owners_are(me, devices), slot, -1), axis=0)
    spots = jnp.arange(devices * first_cap)
    send = jnp.max(jnp.where(mine[None] == spots[:, None], jnp.arange(count)[None], 0), axis=1)
    arrive = (jnp.arange(devices)[:, None] * first_cap + slot % first_cap).reshape(-1)
    handed = jnp.where(relayed & (via == me), (owner % part) * second_cap + second, -1)
    hops = jnp.arange(part * second_cap)
    relay = jnp.max(
        jnp.where(handed.reshape(-1)[None] == hops[:, None], arrive[None], 0), axis=1
    )
    direct = arrive.reshape(devices, count)
    indirect = devices * first_cap + (via % part) * second_cap + second
    where = jnp.where(relayed, indirect, direct).reshape(-1)
    inside = jnp.where(owner == me, labels - me * block_len, -1).reshape(-1)
    hits = inside[None] == jnp.arange(block_len)[:, None]
    return send, relay, jnp.max(jnp.where(hits, where[None], -1), axis=1)


def owners_are(me, devices):
    return (jnp.arange(devices) == me)[:, None]


def pack_relay_kernel(table, arrived, out, sem):
    def fetch(i, carry):
        pltpu.make_async_copy(arrived.at[table[i]], out.at[i], sem).start()
        return carry

    lax.fori_loop(0, out.shape[0], fetch, 0)
    pltpu.make_async_copy(out, out, sem).wait()


def pack_relay(table, arrived):
    return pl.pallas_call(
        pack_relay_kernel,
        out_shape=jax.ShapeDtypeStruct((table.shape[0],) + arrived.shape[1:], arrived.dtype),
        in_specs=[
            pl.BlockSpec(memory_space=pltpu.SMEM),
            pl.BlockSpec(memory_space=pl.ANY),
        ],
        out_specs=pl.BlockSpec(memory_space=pltpu.VMEM),
        scratch_shapes=[pltpu.SemaphoreType.DMA],
        compiler_params=params(),
        name="pack_relay",
    )(table, arrived)


def pack_fine_kernel(table, source, out, sem):
    def send(i, carry):
        pltpu.make_async_copy(source.at[table[i]], out.at[i], sem).start()
        return carry

    lax.fori_loop(0, out.shape[0], send, 0)
    pltpu.make_async_copy(out, out, sem).wait()


def pack_fine(table, fine):
    return pl.pallas_call(
        pack_fine_kernel,
        out_shape=jax.ShapeDtypeStruct((table.shape[0],) + fine.shape[1:], fine.dtype),
        in_specs=[
            pl.BlockSpec(memory_space=pltpu.SMEM),
            pl.BlockSpec(memory_space=pltpu.VMEM),
        ],
        out_specs=pl.BlockSpec(memory_space=pl.ANY),
        scratch_shapes=[pltpu.SemaphoreType.DMA],
        compiler_params=params(),
        name="pack_fine",
    )(table, fine)


def pack_coarse_kernel(table, source, out):
    half = source.shape[-1]

    def step(i, carry):
        out[i, :, :, 0:half] = source[table[2 * i]]
        out[i, :, :, half : 2 * half] = source[table[2 * i + 1]]
        return carry

    lax.fori_loop(0, out.shape[0], step, 0)


def pack_coarse(table, coarse):
    shape = (table.shape[0] // 2,) + coarse.shape[1:3] + (2 * coarse.shape[3],)
    return pl.pallas_call(
        pack_coarse_kernel,
        out_shape=jax.ShapeDtypeStruct(shape, coarse.dtype),
        in_specs=[
            pl.BlockSpec(memory_space=pltpu.SMEM),
            pl.BlockSpec(memory_space=pltpu.VMEM),
        ],
        out_specs=pl.BlockSpec(memory_space=pltpu.VMEM),
        compiler_params=params(),
        name="pack_coarse",
    )(table, coarse)


def refine_kernel(table, pairs, weights, out):
    species, rows, depth = pairs.shape[1:]
    half = depth // 2
    lane = lax.broadcasted_iota(jnp.int32, (species * rows, depth), 1)
    row = lax.broadcasted_iota(jnp.int32, (species, rows, depth), 1)

    def step(c, carry):
        slot = jnp.maximum(table[c], 0)
        block = pairs[slot // 2].reshape(species * rows, depth)
        odd = slot % 2
        block = jnp.where((lane >= half).astype(jnp.int32) == odd, block, 0.0)
        spread = jnp.dot(
            block, weights[...], precision=lax.Precision.HIGHEST,
            preferred_element_type=jnp.float32,
        )
        plain = spread[:, :depth].reshape(species, rows, depth)
        sloped = spread[:, depth:].reshape(species, rows, depth)
        below = jnp.where(row == 0, plain, pltpu.roll(plain, 1, 1))
        above = jnp.where(row == rows - 1, plain, pltpu.roll(plain, rows - 1, 1))
        slope = 0.125 * (above - below)
        for s in range(species):
            out[c, s, pl.ds(0, rows, 2), :] = sloped[s] - slope[s]
            out[c, s, pl.ds(1, rows, 2), :] = sloped[s] + slope[s]
        return carry

    lax.fori_loop(0, out.shape[0], step, 0)


def spread_weights(half):
    depth = 2 * half
    coarse = jnp.arange(half)[:, None]
    fine = jnp.arange(depth)[None, :]
    centre = (fine // 2 == coarse).astype(jnp.float32)
    up = (jnp.minimum(fine // 2 + 1, half - 1) == coarse).astype(jnp.float32)
    down = (jnp.maximum(fine // 2 - 1, 0) == coarse).astype(jnp.float32)
    side = jnp.where(fine % 2 == 1, 0.125, -0.125)
    both = jnp.concatenate([centre, centre + side * (up - down)], axis=1)
    return jnp.concatenate([both, both], axis=0)


def refine(table, pairs, weights):
    species, rows, depth = pairs.shape[1:]
    return pl.pallas_call(
        refine_kernel,
        out_shape=jax.ShapeDtypeStruct(
            (table.shape[0], species, 2 * rows, depth), pairs.dtype
        ),
        in_specs=[
            pl.BlockSpec(memory_space=pltpu.SMEM),
            pl.BlockSpec(memory_space=pltpu.VMEM),
            pl.BlockSpec(memory_space=pltpu.VMEM),
        ],
        out_specs=pl.BlockSpec(memory_space=pltpu.VMEM),
        compiler_params=params(),
        cost_estimate=pl.CostEstimate(
            flops=40_000_000, bytes_accessed=30_000_000, transcendentals=0
        ),
        name="refine",
    )(table, pairs, weights)


def assemble_kernel(table, arrived, passed, interp, out, low, high, sem):
    near = arrived.shape[0]
    planes = out.shape[0]
    rows = out.shape[2]

    def fetch(p, carry):
        slot = table[p]

        @pl.when((slot >= 0) & (slot < near))
        def _():
            pltpu.make_async_copy(arrived.at[slot], out.at[p], sem).start()

        @pl.when(slot >= near)
        def _():
            pltpu.make_async_copy(passed.at[slot - near], out.at[p], sem).start()

        @pl.when(slot < 0)
        def _():
            pltpu.make_async_copy(interp.at[p // 2], out.at[p], sem).start()

        return carry

    lax.fori_loop(0, planes, fetch, 0)
    pltpu.make_async_copy(out, out, sem).wait()

    def edges(p, carry):
        low[p] = out[p, :, 0, :]
        high[p] = out[p, :, rows - 1, :]
        return carry

    lax.fori_loop(0, planes, edges, 0)


def assemble(table, arrived, passed, interp):
    planes = table.shape[0]
    species, rows, depth = arrived.shape[1:]
    edge = jax.ShapeDtypeStruct((planes, species, depth), arrived.dtype)
    return pl.pallas_call(
        assemble_kernel,
        out_shape=(
            jax.ShapeDtypeStruct((planes, species, rows, depth), arrived.dtype),
            edge,
            edge,
        ),
        in_specs=[
            pl.BlockSpec(memory_space=pltpu.SMEM),
            pl.BlockSpec(memory_space=pl.ANY),
            pl.BlockSpec(memory_space=pl.ANY),
            pl.BlockSpec(memory_space=pl.ANY),
        ],
        out_specs=(pl.BlockSpec(memory_space=pltpu.VMEM),) * 3,
        scratch_shapes=[pltpu.SemaphoreType.DMA],
        compiler_params=params(),
        name="assemble",
    )(table, arrived, passed, interp)


def advance_kernel(steps, diffusion, u, before, after, first, last, below, above, flow, out, *edges):
    i = pl.program_id(0)
    block, species, rows, depth = u.shape
    row = lax.broadcasted_iota(jnp.int32, (rows, depth), 0)
    lane = lax.broadcasted_iota(jnp.int32, (rows, depth), 1)

    def plane(x, s):
        return u[x, s]

    for x in range(block):
        v = [flow[x, k] for k in range(3)]
        plus = [jnp.maximum(w, 0.0) for w in v]
        minus = [jnp.maximum(-w, 0.0) for w in v]
        rest = 1.0
        for k in range(3):
            rest = rest - plus[k] - minus[k]
        for s in range(species):
            d = diffusion[s]
            c = u[x, s]
            if x > 0:
                lo = u[x - 1, s]
            else:
                lo = jnp.where(i == 0, first[0, s], before[0, s])
            if x < block - 1:
                hi = u[x + 1, s]
            else:
                hi = jnp.where(i == steps - 1, last[0, s], after[0, s])
            ylo = jnp.where(row == 0, below[x, pl.ds(s, 1), :], pltpu.roll(c, 1, 0))
            yhi = jnp.where(row == rows - 1, above[x, pl.ds(s, 1), :], pltpu.roll(c, rows - 1, 0))
            zlo = jnp.where(lane == 0, c, pltpu.roll(c, 1, 1))
            zhi = jnp.where(lane == depth - 1, c, pltpu.roll(c, depth - 1, 1))
            total = (rest - 6.0 * d) * c
            total = total + (plus[0] + d) * lo + (minus[0] + d) * hi
            total = total + (plus[1] + d) * ylo + (minus[1] + d) * yhi
            total = total + (plus[2] + d) * zlo + (minus[2] + d) * zhi
            out[x, s] = total
            if edges:
                edges[0][x, pl.ds(s, 1), :] = total[0:1]
                edges[1][x, pl.ds(s, 1), :] = total[rows - 1 : rows]


def advance(diffusion, u, first, last, below, above, flow, with_edges):
    planes, species, rows, depth = u.shape
    block = 8 if planes % 8 == 0 else 1
    steps = planes // block
    edge_spec = pl.BlockSpec((block, species, depth), lambda i: (i, 0, 0))
    plane_spec = pl.BlockSpec((1, species, rows, depth), lambda i: (0, 0, 0, 0))
    block_spec = pl.BlockSpec((block, species, rows, depth), lambda i: (i, 0, 0, 0))
    shapes = [jax.ShapeDtypeStruct(u.shape, u.dtype)]
    out_specs = [block_spec]
    if with_edges:
        shapes += [jax.ShapeDtypeStruct((planes, species, depth), u.dtype)] * 2
        out_specs += [edge_spec] * 2
    return pl.pallas_call(
        functools.partial(advance_kernel, steps),
        grid=(steps,),
        out_shape=shapes,
        in_specs=[
            pl.BlockSpec(memory_space=pltpu.SMEM),
            block_spec,
            pl.BlockSpec(
                (1, species, rows, depth), lambda i: (jnp.maximum(i * block - 1, 0), 0, 0, 0)
            ),
            pl.BlockSpec(
                (1, species, rows, depth),
                lambda i: (jnp.minimum(i * block + block, planes - 1), 0, 0, 0),
            ),
            plane_spec,
            plane_spec,
            edge_spec,
            edge_spec,
            pl.BlockSpec((block, 3, rows, depth), lambda i: (i, 0, 0, 0)),
        ],
        out_specs=out_specs,
        compiler_params=params(),
        name="advance",
    )(diffusion, u, u, u, first, last, below, above, flow)


def shift_up(value, axis):
    size = lax.axis_size(axis)
    return lax.ppermute(value, axis, [(i, i + 1) for i in range(size - 1)])


def shift_down(value, axis):
    size = lax.axis_size(axis)
    return lax.ppermute(value, axis, [(i + 1, i) for i in range(size - 1)])


def on_device(old_fine, old_ids, old_coarse, coarse_ids, velocity, diffusion):
    devices = lax.axis_size("dev")
    me = lax.axis_index("dev")
    planes = old_fine.shape[0]
    coarse_planes = old_coarse.shape[0]
    capacity = max(2, 2 * planes // devices)
    coarse_capacity = max(2, 2 * coarse_planes // devices)
    both = jnp.concatenate([old_ids[0], coarse_ids[0]])
    every = lax.all_gather(both, ("grp", "dev"))
    groups = every.reshape(lax.axis_size("grp"), devices, -1)
    here = (jnp.arange(groups.shape[0]) == lax.axis_index("grp"))[:, None, None]
    both_all = jnp.max(jnp.where(here, groups, -1), axis=0)
    labels = both_all[:, :planes]
    coarse_send = send_table(coarse_ids[0], coarse_planes, devices, coarse_capacity)
    coarse_table = receive_table(both_all[:, planes:], coarse_planes, coarse_capacity, me)
    weights = spread_weights(old_coarse.shape[3])
    coarse_out = pack_coarse(coarse_send, old_coarse)
    coarse_in = lax.all_to_all(coarse_out, "dev", split_axis=0, concat_axis=0, tiled=True)

    def padded(fine, coarse):
        send = send_table(old_ids[0], planes, devices, capacity)
        table = receive_table(labels, planes, capacity, me)
        arrived = lax.all_to_all(pack_fine(send, fine), "dev", split_axis=0, concat_axis=0, tiled=True)
        interp = refine(coarse_table, coarse, weights)
        return assemble(table, arrived, arrived, interp)

    if capacity >= 16 and devices % 2 == 0:
        first_cap, second_cap = 5 * capacity // 8, capacity // 4
        plan = functools.partial(
            exchange_plan, block_len=planes, first_cap=first_cap, second_cap=second_cap
        )
        plans = jax.vmap(plan)(groups[:, :, :planes])
        fits = jnp.all(plans[4])
        own = [jnp.max(jnp.where(here, value.astype(jnp.int32), -1), axis=0) for value in plans[:4]]
        own[2] = own[2] > 0
        send, relay, table = plan_tables(
            labels, own + [None], planes, first_cap, second_cap, me
        )
        part = devices // 2
        halves = [list(range(part)), list(range(part, devices))]

        def relayed(fine, coarse):
            arrived = lax.all_to_all(
                pack_fine(send, fine), "dev", split_axis=0, concat_axis=0, tiled=True
            )
            interp = refine(coarse_table, coarse, weights)
            passed = lax.all_to_all(
                pack_relay(relay, arrived), "dev", split_axis=0, concat_axis=0,
                axis_index_groups=halves, tiled=True,
            )
            return assemble(table, arrived, passed, interp)

        u, low, high = lax.cond(fits, relayed, padded, old_fine, coarse_in)
    else:
        u, low, high = padded(old_fine, coarse_in)
    for repeat in range(ITERS):
        first = shift_up(u[-1:], "dev")
        last = shift_down(u[:1], "dev")
        below = shift_up(high, "grp")
        above = shift_down(low, "grp")
        more = repeat < ITERS - 1
        outs = advance(diffusion, u, first, last, below, above, velocity, more)
        if more:
            u, low, high = outs
        else:
            u = outs[0]
    return u


def solution(mesh):
    in_specs = (
        P("dev", None, "grp", None),
        P("grp", "dev"),
        P("dev", None, "grp", None),
        P("grp", "dev"),
        P("dev", None, "grp", None),
        P(),
    )
    out_specs = P("dev", None, "grp", None)
    return jax.shard_map(
        on_device, mesh=mesh, in_specs=in_specs, out_specs=out_specs, check_vma=False
    )
```
